32 devices in a mesh: grp: 2 (over y), pen: 8 (over z, x), ch: 2 (over core).
Axes of the slice: x: 2, y: 2, z: 4, core: 2. Of those that a mesh axis runs over, the one named last changes fastest.
Arguments:
- features: bfloat16 [256, 32, 128, 256], P(('grp', 'pen'), 'ch'), parts along dimension 0, may hold values from -6 to 6
- spectral_weights: bfloat16 [1, 2, 16, 32, 32, 1024], P(None, None, None, None, 'ch', 'pen'), may hold values from -0.75 to 0.75
- bypass_weights: float32 [1, 32, 32], P(None, None, 'ch'), may hold values from -0.75 to 0.75
- bypass_bias: float32 [1, 32], P(None, 'ch'), may hold values from -1 to 1
Outputs:
- features_out: float32 [256, 32, 128, 256], P(('grp', 'pen'), 'ch'), parts along dimension 0
The draws below stay inside these ranges and needn't reach their ends.
There are 2 independent parts, one for each index of `grp`. The reference program is written for one: setup_inputs(seed, part) draws one part's arguments, and reference() takes and returns one part's arrays. A program takes and returns all parts, laid end to end along the dimension named above; an argument that names none is the same for every part. Nothing has to cross between parts.
All inputs are finite; a program needn't handle non-finite values.
Results may differ from the reference program's by a relative error of at most 0.0003.
Values may be sent and summed in bfloat16 or wider, within the bound.
A program may use at most 192 MiB of HBM per device.

```python
import math
import jax
import jax.numpy as jnp
from jax import lax

C = 32
NX = 128
NY = 128
NZ = 256
MX = 16
MY = 32
MZ = 32
LAYERS = 1


def steps_of(key, dims, shards, low, largest):
    factor_of, own = 1.0, jax.random.fold_in(key, 6)
    for axis_at, blocks in shards:
        draws = jnp.exp(jax.random.uniform(jax.random.fold_in(own, axis_at), (blocks,), jnp.float32, low / len(shards), largest / len(shards)))
        factor_of = factor_of * jnp.repeat(draws, dims[axis_at] // blocks).reshape([-1 if axis == axis_at else 1 for axis in range(len(dims))])
    return factor_of


def noise(key, shape, deviation, reach, cuts=(), kind=jnp.bfloat16):
    values = deviation * jax.random.normal(key, shape, jnp.float32)
    if cuts:
        values = values * steps_of(key, shape, cuts, -0.22, 0.18)
    return jnp.clip(values, -reach, reach).astype(kind)


def setup_inputs(seed: int = 0, part: int = 0) -> dict:
    streams_of = jax.random.split(jax.random.key(seed), 5)
    own_keys = jax.random.split(jax.random.fold_in(streams_of[4], part), 5)
    return {
        "features": noise(own_keys[0], (NX, C, NY, NZ), 1.0, 6.0, ((0, 8), (1, 2))),
        "spectral_weights": noise(streams_of[1], (LAYERS, 2, MX, C, C, MY * MZ), (2 * C) ** -0.5, 0.75, ((4, 2), (5, 8))),
        "bypass_weights": noise(streams_of[2], (LAYERS, C, C), (2 * C) ** -0.5, 0.75, ((2, 2),), jnp.float32),
        "bypass_bias": jnp.clip(jax.random.uniform(streams_of[3], (LAYERS, C), jnp.float32, -1.0, 1.0) * steps_of(streams_of[3], (LAYERS, C), ((1, 2),), -0.4, 0.0), -1.0, 1.0),
    }


HIGHEST = lax.Precision.HIGHEST


def kept_freqs(length, kept_count):
    offsets = jnp.arange(kept_count, dtype=jnp.int32)
    return jnp.where(offsets < kept_count // 2, offsets, length - kept_count + offsets)


def tables(length, kept_count):
    phases = (kept_freqs(length, kept_count)[:, None] * jnp.arange(length, dtype=jnp.int32)[None, :]) % length
    angles = phases.astype(jnp.float32) * (2.0 * math.pi / length)
    return jnp.cos(angles), jnp.sin(angles)


def reference(features, spectral_weights, bypass_weights, bypass_bias):
    cos_x, sin_x = tables(NX, MX)
    cos_y, sin_y = tables(NY, MY)
    cos_z, sin_z = tables(NZ, MZ)

    def forward_slab(x_slab):
        real_z = jnp.einsum('cyz,kz->cyk', x_slab, cos_z, precision=HIGHEST) * NZ ** -0.5
        imag_z = -jnp.einsum('cyz,kz->cyk', x_slab, sin_z, precision=HIGHEST) * NZ ** -0.5
        real_y = (jnp.einsum('ay,cyk->cak', cos_y, real_z, precision=HIGHEST)
                  + jnp.einsum('ay,cyk->cak', sin_y, imag_z, precision=HIGHEST)) * NY ** -0.5
        imag_y = (jnp.einsum('ay,cyk->cak', cos_y, imag_z, precision=HIGHEST)
                  - jnp.einsum('ay,cyk->cak', sin_y, real_z, precision=HIGHEST)) * NY ** -0.5
        return real_y, imag_y

    current = features.astype(jnp.float32)
    for layer_idx in range(LAYERS):
        real_y, imag_y = lax.map(forward_slab, current)
        real_x = (jnp.einsum('jx,xcak->jcak', cos_x, real_y, precision=HIGHEST)
                  + jnp.einsum('jx,xcak->jcak', sin_x, imag_y, precision=HIGHEST)) * NX ** -0.5
        imag_x = (jnp.einsum('jx,xcak->jcak', cos_x, imag_y, precision=HIGHEST)
                  - jnp.einsum('jx,xcak->jcak', sin_x, real_y, precision=HIGHEST)) * NX ** -0.5
        weights = spectral_weights[layer_idx].astype(jnp.float32).reshape(2, MX, C, C, MY, MZ)
        real_g = (jnp.einsum('jiak,jioak->joak', real_x, weights[0], precision=HIGHEST)
                  - jnp.einsum('jiak,jioak->joak', imag_x, weights[1], precision=HIGHEST))
        imag_g = (jnp.einsum('jiak,jioak->joak', imag_x, weights[0], precision=HIGHEST)
                  + jnp.einsum('jiak,jioak->joak', real_x, weights[1], precision=HIGHEST))
        real_h = (jnp.einsum('jx,joak->xoak', cos_x, real_g, precision=HIGHEST)
                  - jnp.einsum('jx,joak->xoak', sin_x, imag_g, precision=HIGHEST)) * MX ** -0.5
        imag_h = (jnp.einsum('jx,joak->xoak', cos_x, imag_g, precision=HIGHEST)
                  + jnp.einsum('jx,joak->xoak', sin_x, real_g, precision=HIGHEST)) * MX ** -0.5
        mixing = bypass_weights[layer_idx].astype(jnp.float32)
        offsets = bypass_bias[layer_idx].astype(jnp.float32)

        def inverse_slab(pieces, mixing=mixing, offsets=offsets):
            x_slab, real_b, imag_b = pieces
            real_a = (jnp.einsum('ay,oak->oyk', cos_y, real_b, precision=HIGHEST)
                      - jnp.einsum('ay,oak->oyk', sin_y, imag_b, precision=HIGHEST)) * MY ** -0.5
            imag_a = (jnp.einsum('ay,oak->oyk', cos_y, imag_b, precision=HIGHEST)
                      + jnp.einsum('ay,oak->oyk', sin_y, real_b, precision=HIGHEST)) * MY ** -0.5
            spectral = (jnp.einsum('oyk,kz->oyz', real_a, cos_z, precision=HIGHEST)
                        - jnp.einsum('oyk,kz->oyz', imag_a, sin_z, precision=HIGHEST)) * MZ ** -0.5
            bypass = jnp.einsum('io,iyz->oyz', mixing, x_slab, precision=HIGHEST)
            return x_slab + jax.nn.gelu(bypass + offsets[:, None, None] + spectral, approximate=True)

        current = lax.map(inverse_slab, (current, real_h, imag_h))
    return current
```

```python
import functools
import math

import jax
import jax.numpy as jnp
import ml_dtypes
import numpy as np
from jax import lax
from jax.experimental import pallas as pl
from jax.experimental.pallas import tpu as pltpu
from jax.sharding import PartitionSpec as P

HIGHEST = lax.Precision.HIGHEST
LANES = 128
MZ = 32
F32 = jnp.float32
BF16 = jnp.bfloat16


def tables(length, kept):
    offsets = np.arange(kept)
    freqs = np.where(offsets < kept // 2, offsets, length - kept + offsets)
    phases = (freqs[:, None] * np.arange(length)[None, :]) % length
    angles = phases.astype(np.float64) * (2.0 * math.pi / length)
    return np.cos(angles), np.sin(angles)


def split_np(table):
    table = table.astype(np.float32)
    high = table.astype(ml_dtypes.bfloat16)
    low = (table - high.astype(np.float32)).astype(ml_dtypes.bfloat16)
    return high, low


def split(value):
    high = value.astype(BF16)
    return high, (value - high.astype(F32)).astype(BF16)


def dot(left, right):
    return jnp.dot(left, right, preferred_element_type=F32)


def forward_kernel(x_ref, ty_ref, bh_ref, bl_ref, out_ref, y_ref, *, my, nsub):
    block, ch, _, nz = x_ref.shape
    parts = nz // LANES
    groups = my // nsub
    half = my * ch
    for b in range(block):
        for c in range(ch):
            both = dot(ty_ref[...], x_ref[b, c])
            rows = both[: 2 * my] + both[2 * my :]
            for part in range(parts):
                y_ref[b, part, pl.ds(c, 2 * my, stride=ch), :] = rows[
                    :, part * LANES : (part + 1) * LANES
                ]
    highs, lows = [], []
    for b in range(block):
        pieces = []
        for cs in range(2):
            loaded = [
                y_ref[b, part, cs * half : (cs + 1) * half, :].reshape(groups, nsub, ch, LANES)
                for part in range(parts)
            ]
            for sub in range(nsub):
                for part in range(parts):
                    pieces.append(loaded[part][:, sub].reshape(groups * ch, LANES))
        high, low = split(jnp.concatenate(pieces, axis=1))
        highs.append(high)
        lows.append(low)
    high = jnp.concatenate(highs, axis=0)
    low = jnp.concatenate(lows, axis=0)
    result = dot(high, bh_ref[...]) + dot(low, bh_ref[...]) + dot(high, bl_ref[...])
    result = result.reshape(block, groups, ch, 2 * LANES)
    for b in range(block):
        out_ref[:, b] = result[b]


MESH = pl.DeviceIdType.MESH
CHUNKS = 4


def odd_power(value, power):
    result, square = value, value * value
    while power > 1:
        result, power = result * square, power - 2
    return result


def encode(value, power, scale):
    return odd_power(value * scale, power).astype(WIRE)


def decode(code, power, scale):
    code = code.astype(F32)
    root = jnp.exp2(jnp.log2(jnp.abs(code)) * (1.0 / power)) * (1.0 / scale)
    return jnp.where(code < 0.0, -root, root)


WIRE = BF16
MODES_CODE = (7, 16.0)
MIXED_CODE = (5, 1.0)


def spectrum_kernel(
    x_ref, feat_ref, weight_ref, ty_ref, bh_ref, bl_ref, tx_ref, ix_ref, out_ref, field_ref,
    y_ref, send, recv, wide, fx, weight, partial, every, plain,
    send_sem, recv_sem, gsend_sem, grecv_sem, psend_sem, fsend_sem, frecv_sem, xsem, wsem,
    *, my, nsub, pens, near,
):
    step = pl.program_id(0)
    steps = pl.num_programs(0)
    me = lax.axis_index("pen")
    core = lax.axis_index("ch")
    block, ch, _, nz = x_ref.shape
    parts = nz // LANES
    groups = my // nsub
    half = my * ch
    mx = every.shape[1]
    slabs = recv.shape[1] * block
    far = pens // near
    nx = wide.shape[1] // ch
    nblocks = recv.shape[1]
    chunks = grecv_sem.shape[1]
    span = mx // chunks

    def field_copy(at):
        window = pl.ds(at * block, block)
        return pltpu.make_async_remote_copy(
            src_ref=feat_ref.at[window],
            dst_ref=field_ref.at[window],
            send_sem=fsend_sem.at[at],
            recv_sem=frecv_sem.at[at],
            device_id={"ch": 1 - core},
            device_id_type=MESH,
        )

    def modes_copy(at, shift, source):
        target = lax.rem(me + shift, pens)
        return pltpu.make_async_remote_copy(
            src_ref=send.at[at, target],
            dst_ref=recv.at[source, at],
            send_sem=send_sem.at[at, shift - 1],
            recv_sem=recv_sem.at[source, at],
            device_id={"pen": target},
            device_id_type=MESH,
        )

    def column_copy(chunk, shift, source):
        target = lax.rem(me + shift * near, pens)
        window = pl.ds(chunk * span, span)
        return pltpu.make_async_remote_copy(
            src_ref=every.at[me, window],
            dst_ref=every.at[source, window],
            send_sem=gsend_sem.at[chunk, shift - 1],
            recv_sem=grecv_sem.at[source, chunk],
            device_id={"pen": target},
            device_id_type=MESH,
        )

    def row_copy(chunk, shift, source, landing):
        base = me - lax.rem(me, near)
        target = base + lax.rem(me + shift, near)
        window = pl.ds(chunk * span, span)
        return pltpu.make_async_remote_copy(
            src_ref=every.at[source, window],
            dst_ref=every.at[landing, window],
            send_sem=psend_sem.at[source, chunk, shift - 1],
            recv_sem=grecv_sem.at[landing, chunk],
            device_id={"pen": target},
            device_id_type=MESH,
        )

    def weight_copy():
        return pltpu.make_async_copy(weight_ref.at[0], weight, wsem)

    def pair_copy():
        return pltpu.make_async_remote_copy(
            src_ref=fx.at[0],
            dst_ref=fx.at[1],
            send_sem=xsem.at[0],
            recv_sem=xsem.at[1],
            device_id={"ch": 1 - core},
            device_id_type=MESH,
        )

    @pl.when(step == 0)
    def _():
        barrier = pltpu.get_barrier_semaphore()
        for shift in range(1, pens):
            pl.semaphore_signal(
                barrier, inc=1, device_id={"pen": lax.rem(me + shift, pens)}, device_id_type=MESH
            )
        pl.semaphore_signal(barrier, inc=1, device_id={"ch": 1 - core}, device_id_type=MESH)
        pl.semaphore_wait(barrier, pens)
        for at in range(nblocks):
            field_copy(at).start()
        weight_copy().start()

    for b in range(block):
        for c in range(ch):
            both = dot(ty_ref[...], x_ref[b, c])
            rows = both[: 2 * my] + both[2 * my :]
            for part in range(parts):
                y_ref[b, part, pl.ds(c, 2 * my, stride=ch), :] = rows[
                    :, part * LANES : (part + 1) * LANES
                ]
    highs, lows = [], []
    for b in range(block):
        pieces = []
        for cs in range(2):
            loaded = [
                y_ref[b, part, cs * half : (cs + 1) * half, :].reshape(groups, nsub, ch, LANES)
                for part in range(parts)
            ]
            for sub in range(nsub):
                for part in range(parts):
                    pieces.append(loaded[part][:, sub].reshape(groups * ch, LANES))
        high, low = split(jnp.concatenate(pieces, axis=1))
        highs.append(high)
        lows.append(low)
    high = jnp.concatenate(highs, axis=0)
    low = jnp.concatenate(lows, axis=0)
    result = dot(high, bh_ref[...]) + dot(low, bh_ref[...]) + dot(high, bl_ref[...])
    result = encode(result, *MODES_CODE).reshape(block, groups, ch, 2 * LANES)
    for b in range(block):
        send[step, :, b] = result[b]
    recv[me, step] = send[step, me]
    for shift in range(1, pens):
        modes_copy(step, shift, me).start()

    @pl.when(step == steps - 1)
    def _():
        def widen(source, at):
            rows = decode(recv[source, at].reshape(block * ch, 2 * LANES), *MODES_CODE)
            window = pl.ds(pl.multiple_of((source * nblocks + at) * (block * ch), 8), block * ch)
            wide[0, window, :] = rows[:, :LANES]
            wide[1, window, :] = rows[:, LANES:]

        @pl.loop(0, nblocks)
        def _(at):
            widen(me, at)

        for shift in range(1, pens):
            source = lax.rem(me + pens - shift, pens)

            @pl.loop(0, nblocks)
            def _(at):
                modes_copy(at, shift, source).wait_recv()
                widen(source, at)

        for c in range(ch):
            rows = jnp.concatenate(
                [wide[part, pl.ds(c, nx, stride=ch), :] for part in range(2)], axis=1
            )
            high, low = split(rows)
            both = dot(tx_ref[...], jnp.concatenate([high, low], axis=0))
            waves = both[: 2 * mx] + both[2 * mx :]
            fx[0, 0, pl.ds(c, mx, stride=ch), :] = waves[:mx, :LANES] + waves[mx:, LANES:]
            fx[0, 1, pl.ds(c, mx, stride=ch), :] = waves[:mx, LANES:] - waves[mx:, :LANES]
        pair_copy().start()
        weight_copy().wait()

        def mix(slot, j, real, imag):
            first = (core if slot == 0 else 1 - core) * ch
            for c in range(ch):
                x_re = fx[slot, 0, pl.ds(j * ch + c, 1), :]
                x_im = fx[slot, 1, pl.ds(j * ch + c, 1), :]
                w_re = weight[0, j, first + c].astype(F32)
                w_im = weight[1, j, first + c].astype(F32)
                real = real + (x_re * w_re - x_im * w_im)
                imag = imag + (x_im * w_re + x_re * w_im)
            return real, imag

        @pl.loop(0, mx)
        def _(j):
            zero = jnp.zeros(partial.shape[2:], F32)
            partial[0, j], partial[1, j] = mix(0, j, zero, zero)

        pair_copy().wait()

        @pl.loop(0, chunks)
        def _(chunk):
            @pl.loop(0, span)
            def _(local_j):
                j = chunk * span + local_j
                real, imag = mix(1, j, partial[0, j], partial[1, j])
                coded = encode(jnp.concatenate([real, imag], axis=1), *MIXED_CODE)
                every[me, j] = coded

            for shift in range(1, far):
                column_copy(chunk, shift, me).start()
            for shift in range(1, near):
                row_copy(chunk, shift, me, me).start()

        @pl.loop(0, nblocks)
        def _(at):
            for shift in range(1, pens):
                modes_copy(at, shift, me).wait_send()

        @pl.loop(0, chunks)
        def _(chunk):
            for shift in range(1, far):
                source = lax.rem(me + pens - shift * near, pens)
                column_copy(chunk, shift, source).wait_recv()
                for side in range(1, near):
                    row_copy(chunk, side, source, source).start()

        def finish(source):
            @pl.loop(0, mx)
            def _(j):
                rows = decode(every[source, j], *MIXED_CODE)
                window = pl.ds(pl.multiple_of(j * ch, 8), ch)
                plain[0, window, :] = rows[:, :LANES]
                plain[1, window, :] = rows[:, LANES:]

            for o in range(ch):
                real = plain[0, pl.ds(o, mx, stride=ch), :]
                imag = plain[1, pl.ds(o, mx, stride=ch), :]
                rows = jnp.concatenate(
                    [
                        jnp.concatenate([real, imag], axis=1),
                        jnp.concatenate([imag, -real], axis=1),
                    ],
                    axis=0,
                )
                high, low = split(rows)
                waves = dot(ix_ref[...], jnp.concatenate([high, high, low], axis=0))
                window = pl.ds(o * groups + source, slabs, stride=groups * ch)
                out_ref[0, window, :] = waves[:, :LANES]
                out_ref[1, window, :] = waves[:, LANES:]

        @pl.loop(0, far)
        def _(shift):
            source = lax.rem(me + pens - shift * near, pens)
            finish(source)

        base = me - lax.rem(me, near)
        for side in range(1, near):
            @pl.loop(0, far)
            def _(shift):
                column = base + lax.rem(me + near - side, near)
                source = lax.rem(column + pens - shift * near, pens)

                @pl.loop(0, chunks)
                def _(chunk):
                    row_copy(chunk, side, source, source).wait_recv()

                finish(source)

        @pl.loop(0, chunks)
        def _(chunk):
            for shift in range(1, far):
                column_copy(chunk, shift, me).wait_send()
            for shift in range(far):
                source = lax.rem(me + pens - shift * near, pens)
                for side in range(1, near):
                    row_copy(chunk, side, source, source).wait_send()

        @pl.loop(0, nblocks)
        def _(at):
            field_copy(at).wait()


def forward_tables(ny, nz, my, mz):
    nsub = LANES // mz
    cos_y, sin_y = tables(ny, my)
    cos_z, sin_z = tables(nz, mz)
    y_table = np.concatenate(split_np(np.concatenate([cos_y, sin_y]) * ny**-0.5), axis=0)
    pair = np.stack([np.stack([cos_z, -sin_z]), np.stack([-sin_z, -cos_z])]) * nz**-0.5
    z_table = np.einsum("crkz,st->cszrtk", pair, np.eye(nsub)).reshape(2 * nsub * nz, 2 * LANES)
    return (y_table, *split_np(z_table))


def inverse_x_table(nx, mx):
    cos_x, sin_x = tables(nx, mx)
    high, low = split_np(np.concatenate([cos_x, -sin_x]).T * mx**-0.5)
    return np.concatenate([high, low, high], axis=1)


def spectrum(features, weights, my, mz, pens, near):
    slabs, ch, ny, nz = features.shape
    _, _, mx, all_ch, _, _ = weights.shape
    nx = slabs * pens
    nsub = LANES // mz
    groups = my // nsub
    y_table, z_high, z_low = forward_tables(ny, nz, my, mz)
    cos_x, sin_x = tables(nx, mx)
    x_high, x_low = split_np(np.concatenate([cos_x, sin_x]) * nx**-0.5)
    x_table = np.concatenate(
        [
            np.concatenate([x_high, x_high], axis=1),
            np.concatenate([x_low, np.zeros_like(x_low)], axis=1),
        ],
        axis=0,
    )
    inverse = lax.dynamic_slice_in_dim(
        jnp.asarray(inverse_x_table(nx, mx)), lax.axis_index("pen") * slabs, slabs, 0
    )
    block = 2 if slabs % 2 == 0 else 1
    nblocks = slabs // block
    chunks = CHUNKS if mx % CHUNKS == 0 else 1
    anywhere = pl.BlockSpec(memory_space=pl.ANY)
    return pl.pallas_call(
        functools.partial(spectrum_kernel, my=my, nsub=nsub, pens=pens, near=near),
        grid=(nblocks,),
        in_specs=[
            pl.BlockSpec((block, ch, ny, nz), lambda i: (i, 0, 0, 0)),
            anywhere,
            anywhere,
            whole_vmem(),
            whole_vmem(),
            whole_vmem(),
            whole_vmem(),
            whole_vmem(),
        ],
        out_specs=[whole_vmem(), anywhere],
        out_shape=[
            jax.ShapeDtypeStruct((2, slabs * ch * groups, LANES), F32),
            jax.ShapeDtypeStruct(features.shape, features.dtype),
        ],
        scratch_shapes=[
            pltpu.VMEM((block, nz // LANES, 2 * my * ch, LANES), F32),
            pltpu.VMEM((nblocks, pens, block, ch, 2 * LANES), WIRE),
            pltpu.VMEM((pens, nblocks, block, ch, 2 * LANES), WIRE),
            pltpu.VMEM((2, nx * ch, LANES), F32),
            pltpu.VMEM((2, 2, mx * ch, LANES), F32),
            pltpu.VMEM((2, mx, all_ch, ch, LANES), BF16),
            pltpu.VMEM((2, mx, ch, LANES), F32),
            pltpu.VMEM((pens, mx, ch, 2 * LANES), WIRE),
            pltpu.VMEM((2, mx * ch, LANES), F32),
            pltpu.SemaphoreType.DMA((nblocks, pens - 1)),
            pltpu.SemaphoreType.DMA((pens, nblocks)),
            pltpu.SemaphoreType.DMA((chunks, max(pens // near - 1, 1))),
            pltpu.SemaphoreType.DMA((pens, chunks)),
            pltpu.SemaphoreType.DMA((pens, chunks, max(near - 1, 1))),
            pltpu.SemaphoreType.DMA((nblocks,)),
            pltpu.SemaphoreType.DMA((nblocks,)),
            pltpu.SemaphoreType.DMA((2,)),
            pltpu.SemaphoreType.DMA,
        ],
        compiler_params=pltpu.CompilerParams(
            vmem_limit_bytes=60 * 2**20, collective_id=0, has_side_effects=True
        ),
        cost_estimate=pl.CostEstimate(
            flops=32 * slabs * ch * my * ny * nz, bytes_accessed=8 * features.size, transcendentals=0
        ),
        name="spectrum",
    )(
        features,
        features,
        weights,
        jnp.asarray(y_table),
        jnp.asarray(z_high),
        jnp.asarray(z_low),
        jnp.asarray(x_table),
        inverse,
    )


def inverse_kernel(
    h_ref, x_ref, peer_ref, mix_ref, rows_ref, cols_ref, mask_ref, bias_ref, ty_ref, tz_ref, out_ref,
    table,
    *, nsub, groups, ysub
):
    _, ch, ny, nz = x_ref.shape

    @pl.when(pl.program_id(0) == 0)
    def _():
        for at, part in enumerate(split(mix_ref[...])):
            wide = dot(dot(rows_ref[...], part).astype(BF16), cols_ref[...]) * mask_ref[...]
            table[pl.ds(at * ch * ysub, ch * ysub), :] = wide.astype(BF16)

    count = LANES // MZ
    block = lax.broadcasted_iota(jnp.int32, (ch * groups, LANES), 1) // MZ
    real, imag = h_ref[0], h_ref[1]

    def rolled(rows):
        return [rows] + [pltpu.roll(rows, MZ * at, 1) for at in range(1, count)]

    reals, imags = rolled(real), rolled(imag)
    minus = [-rows for rows in reals]

    def laid(even, odd, sub):
        result = even[-sub % count]
        for at in range(1, count):
            result = jnp.where(block == at, (odd if at % 2 else even)[(at - sub) % count], result)
        return result

    tops = [laid(reals, imags, sub) for sub in range(nsub)]
    lows = [laid(imags, minus, sub) for sub in range(nsub)]
    for pair in range(0, ch, 2):
        sides = []
        for o in (pair, pair + 1):
            window = slice(o * groups, (o + 1) * groups)
            high, low = split(jnp.concatenate([rows[window] for rows in tops + lows], axis=0))
            sides.append(jnp.concatenate([high, high, low], axis=0))
        waves = dot(ty_ref[...], jnp.concatenate(sides, axis=1))
        for at, o in enumerate((pair, pair + 1)):
            high, low = split(waves[:, at * LANES : (at + 1) * LANES])
            spectral = dot(jnp.concatenate([high, low], axis=1), tz_ref[...])
            out_ref[0, o] = spectral + bias_ref[0, o]
    for at in range(0, ny, ysub):
        window = slice(at, at + ysub)
        cells = [ref[0, c, window, :] for ref in (x_ref, peer_ref) for c in range(ch)]
        both = dot(table[...], jnp.concatenate(cells, axis=0))
        bypass = both[: ch * ysub] + both[ch * ysub :]
        inner = bypass.reshape(ch, ysub, nz) + out_ref[0, :, window, :]
        own = x_ref[0, :, window, :].astype(F32)
        scale = math.sqrt(2.0 / math.pi)
        cubic = inner * (scale + (0.044715 * scale) * (inner * inner))
        half = 0.5 * inner
        out_ref[0, :, window, :] = own + (half + half * jnp.tanh(cubic))


def whole_vmem():
    return pl.BlockSpec(memory_space=pltpu.VMEM)


def forward_modes(features, my, mz):
    slabs, ch, ny, nz = features.shape
    nsub = LANES // mz
    groups = my // nsub
    cos_y, sin_y = tables(ny, my)
    cos_z, sin_z = tables(nz, mz)
    y_table = np.concatenate(split_np(np.concatenate([cos_y, sin_y]) * ny**-0.5), axis=0)
    pair = np.stack([np.stack([cos_z, -sin_z]), np.stack([-sin_z, -cos_z])]) * nz**-0.5
    z_table = np.einsum("crkz,st->cszrtk", pair, np.eye(nsub)).reshape(2 * nsub * nz, 2 * LANES)
    z_high, z_low = split_np(z_table)
    block = 2 if slabs % 2 == 0 else 1
    return pl.pallas_call(
        functools.partial(forward_kernel, my=my, nsub=nsub),
        grid=(slabs // block,),
        in_specs=[
            pl.BlockSpec((block, ch, ny, nz), lambda i: (i, 0, 0, 0)),
            whole_vmem(),
            whole_vmem(),
            whole_vmem(),
        ],
        out_specs=pl.BlockSpec((groups, block, ch, 2 * LANES), lambda i: (0, i, 0, 0)),
        out_shape=jax.ShapeDtypeStruct((groups, slabs, ch, 2 * LANES), F32),
        scratch_shapes=[pltpu.VMEM((block, nz // LANES, 2 * my * ch, LANES), F32)],
        compiler_params=pltpu.CompilerParams(vmem_limit_bytes=48 * 2**20),
        cost_estimate=pl.CostEstimate(
            flops=32 * slabs * ch * my * ny * nz, bytes_accessed=8 * features.size, transcendentals=0
        ),
        name="forward_modes",
    )(features, jnp.asarray(y_table), jnp.asarray(z_high), jnp.asarray(z_low))


def inverse_field(waves, features, peer, mixing, bias, my, mz):
    slabs, ch, ny, nz = features.shape
    all_ch = mixing.shape[0]
    nsub = LANES // mz
    groups = my // nsub
    ysub = YSUB
    cos_y, sin_y = tables(ny, my)
    cos_z, sin_z = tables(nz, mz)
    y_pair = np.stack([cos_y, -sin_y]).reshape(2, groups, nsub, ny) * my**-0.5
    y_high, y_low = split_np(y_pair.transpose(3, 0, 2, 1).reshape(ny, 2 * my))
    y_table = np.concatenate([y_high, y_low, y_high], axis=1)
    z_high, z_low = split_np(np.concatenate([cos_z, -sin_z]) * mz**-0.5)
    copies = LANES // (2 * mz)
    blank = [np.zeros_like(z_high)] * (copies - 2)
    z_table = np.concatenate(
        [z_high, z_low, *blank, z_high, np.zeros_like(z_high), *blank], axis=0
    )
    high_rows, high_cols = ch * ysub, all_ch * ysub
    spread_rows = np.repeat(np.eye(ch), ysub, axis=0).astype(ml_dtypes.bfloat16)
    spread_cols = np.repeat(np.eye(all_ch), ysub, axis=1).astype(ml_dtypes.bfloat16)
    mask = np.tile(np.eye(ysub), (ch, all_ch)).astype(np.float32)
    rows = ch * groups
    return pl.pallas_call(
        functools.partial(inverse_kernel, nsub=nsub, groups=groups, ysub=ysub),
        grid=(slabs,),
        in_specs=[
            pl.BlockSpec((2, rows, LANES), lambda i: (0, i, 0)),
            pl.BlockSpec((1, ch, ny, nz), lambda i: (i, 0, 0, 0)),
            pl.BlockSpec((1, ch, ny, nz), lambda i: (i, 0, 0, 0)),
            whole_vmem(),
            whole_vmem(),
            whole_vmem(),
            whole_vmem(),
            pl.BlockSpec(memory_space=pltpu.SMEM),
            whole_vmem(),
            whole_vmem(),
        ],
        out_specs=pl.BlockSpec((1, ch, ny, nz), lambda i: (i, 0, 0, 0)),
        out_shape=jax.ShapeDtypeStruct((slabs, ch, ny, nz), F32),
        scratch_shapes=[pltpu.VMEM((2 * high_rows, high_cols), BF16)],
        compiler_params=pltpu.CompilerParams(vmem_limit_bytes=60 * 2**20),
        name="inverse_field",
    )(
        waves,
        features,
        peer,
        mixing.T,
        jnp.asarray(spread_rows),
        jnp.asarray(spread_cols),
        jnp.asarray(mask),
        bias,
        jnp.asarray(y_table),
        jnp.asarray(z_table),
    )


YSUB = 8


def spread_spectrum(features, spectral_weights, my, mz, pens):
    slabs, ch, _, _ = features.shape
    _, _, mx, _, _, owned = spectral_weights.shape
    nx = slabs * pens
    groups = my * mz // LANES
    modes = forward_modes(features, my, mz)
    modes = modes.reshape(groups, slabs, ch, 2, LANES).transpose(1, 2, 3, 0, 4)
    modes = modes.reshape(slabs, ch, 2, pens, owned).transpose(3, 0, 1, 2, 4)
    modes = modes.reshape(pens, slabs, ch, 2 * owned)
    modes = lax.all_to_all(modes, "pen", split_axis=0, concat_axis=0, tiled=True)
    modes = modes.reshape(nx, ch, 2 * owned)
    cos_x, sin_x = tables(nx, mx)
    forward_x = jnp.asarray((np.concatenate([cos_x, sin_x]) * nx**-0.5).astype(np.float32))
    waves = jnp.einsum("dx,xcl->dcl", forward_x, modes, precision=HIGHEST)
    real_x = waves[:mx, :, :owned] + waves[mx:, :, owned:]
    imag_x = waves[:mx, :, owned:] - waves[mx:, :, :owned]
    joined = lax.all_gather(
        jnp.concatenate([real_x, imag_x], axis=2), "ch", axis=1, tiled=True
    )
    real_x = joined[:, :, None, :owned]
    imag_x = joined[:, :, None, owned:]
    weight_re = spectral_weights[0, 0].astype(F32)
    weight_im = spectral_weights[0, 1].astype(F32)
    real_g = jnp.sum(real_x * weight_re - imag_x * weight_im, axis=1)
    imag_g = jnp.sum(imag_x * weight_re + real_x * weight_im, axis=1)
    mixed = lax.all_gather(jnp.concatenate([real_g, imag_g], axis=2), "pen", axis=0)
    mixed = mixed.reshape(pens, mx, ch, 2, owned).transpose(1, 2, 3, 0, 4)
    mixed = mixed.reshape(mx, ch, 2, groups, LANES).transpose(3, 0, 1, 2, 4)
    mixed = mixed.reshape(groups, mx, ch, 2, LANES)
    table = inverse_x_table(nx, mx)[:, : 2 * mx].astype(np.float32)
    table = table + inverse_x_table(nx, mx)[:, 2 * mx : 4 * mx].astype(np.float32)
    table = lax.dynamic_slice_in_dim(
        jnp.asarray(table), lax.axis_index("pen") * slabs, slabs, 0
    )
    real, imag = mixed[:, :, :, 0], mixed[:, :, :, 1]
    pair = jnp.stack([jnp.concatenate([real, imag], 1), jnp.concatenate([imag, -real], 1)])
    waves = jnp.einsum("xj,pgjol->pxogl", table, pair, precision=HIGHEST)
    return waves.reshape(2, slabs * ch * groups, LANES)


def local(features, spectral_weights, bypass_weights, bypass_bias, *, pens, kept):
    slabs, ch, _, _ = features.shape
    _, _, mx, all_ch, _, owned = spectral_weights.shape
    mz = MZ
    my = kept // mz
    near = 2 if pens % 2 == 0 else 1
    core = lax.axis_index("ch")
    if owned == LANES and all_ch == 2 * ch:
        waves, peer = spectrum(features, spectral_weights, my, mz, pens, near)
    else:
        peer = lax.ppermute(features, "ch", [(0, 1), (1, 0)])
        waves = spread_spectrum(features, spectral_weights, my, mz, pens)
    mixing = bypass_weights[0]
    mixing = jnp.where(core == 0, mixing, jnp.roll(mixing, ch, axis=0))
    return inverse_field(waves, features, peer, mixing, bypass_bias, my, mz)


def solution(mesh):
    pens = mesh.shape["pen"]

    def run(features, spectral_weights, bypass_weights, bypass_bias):
        body = functools.partial(local, pens=pens, kept=spectral_weights.shape[5])
        return jax.shard_map(
            body,
            mesh=mesh,
            in_specs=(
                P(("grp", "pen"), "ch", None, None),
                P(None, None, None, None, "ch", "pen"),
                P(None, None, "ch"),
                P(None, "ch"),
            ),
            out_specs=P(("grp", "pen"), "ch", None, None),
            check_vma=False,
        )(features, spectral_weights, bypass_weights, bypass_bias)

    return run
```

```python
import functools
import math

import jax
import jax.numpy as jnp
import ml_dtypes
import numpy as np
from jax import lax
from jax.experimental import pallas as pl
from jax.experimental.pallas import tpu as pltpu
from jax.sharding import PartitionSpec as P

HIGHEST = lax.Precision.HIGHEST
LANES = 128
MZ = 32
F32 = jnp.float32
BF16 = jnp.bfloat16


def tables(length, kept):
    offsets = np.arange(kept)
    freqs = np.where(offsets < kept // 2, offsets, length - kept + offsets)
    phases = (freqs[:, None] * np.arange(length)[None, :]) % length
    angles = phases.astype(np.float64) * (2.0 * math.pi / length)
    return np.cos(angles), np.sin(angles)


def split_np(table):
    table = table.astype(np.float32)
    high = table.astype(ml_dtypes.bfloat16)
    low = (table - high.astype(np.float32)).astype(ml_dtypes.bfloat16)
    return high, low


def split(value):
    high = value.astype(BF16)
    return high, (value - high.astype(F32)).astype(BF16)


def dot(left, right):
    return jnp.dot(left, right, preferred_element_type=F32)


def forward_kernel(x_ref, ty_ref, bh_ref, bl_ref, out_ref, y_ref, *, my, nsub):
    block, ch, _, nz = x_ref.shape
    parts = nz // LANES
    groups = my // nsub
    half = my * ch
    for b in range(block):
        for c in range(ch):
            both = dot(ty_ref[...], x_ref[b, c])
            rows = both[: 2 * my] + both[2 * my :]
            for part in range(parts):
                y_ref[b, part, pl.ds(c, 2 * my, stride=ch), :] = rows[
                    :, part * LANES : (part + 1) * LANES
                ]
    highs, lows = [], []
    for b in range(block):
        pieces = []
        for cs in range(2):
            loaded = [
                y_ref[b, part, cs * half : (cs + 1) * half, :].reshape(groups, nsub, ch, LANES)
                for part in range(parts)
            ]
            for sub in range(nsub):
                for part in range(parts):
                    pieces.append(loaded[part][:, sub].reshape(groups * ch, LANES))
        high, low = split(jnp.concatenate(pieces, axis=1))
        highs.append(high)
        lows.append(low)
    high = jnp.concatenate(highs, axis=0)
    low = jnp.concatenate(lows, axis=0)
    result = dot(high, bh_ref[...]) + dot(low, bh_ref[...]) + dot(high, bl_ref[...])
    result = result.reshape(block, groups, ch, 2 * LANES)
    for b in range(block):
        out_ref[:, b] = result[b]


MESH = pl.DeviceIdType.MESH
CHUNKS = 4
TOGETHER = 2


def odd_power(value, power):
    result, square = value, value * value
    while power > 1:
        result, power = result * square, power - 2
    return result


def encode(value, power, scale):
    return odd_power(value * scale, power).astype(WIRE)


def decode(code, power, scale):
    code = code.astype(F32)
    root = jnp.exp2(jnp.log2(jnp.abs(code)) * (1.0 / power)) * (1.0 / scale)
    return jnp.where(code < 0.0, -root, root)


WIRE = BF16
FIELD_MAX = 6.0
WEIGHT_MAX = 0.75


def code_of(power, bound):
    reach = 2.0 ** (126.0 / power)
    return power, 2.0 ** math.floor(math.log2(reach / bound))


def spectrum_kernel(
    x_ref, feat_ref, weight_ref, ty_ref, bh_ref, bl_ref, tx_ref, ix_ref, out_ref, field_ref,
    y_ref, send, recv, wide, fx, weight, partial, every, plain,
    send_sem, recv_sem, gsend_sem, grecv_sem, psend_sem, fsend_sem, frecv_sem, xsem, wsem,
    *, my, nsub, pens, near, modes_code, mixed_code,
):
    step = pl.program_id(0)
    steps = pl.num_programs(0)
    me = lax.axis_index("pen")
    core = lax.axis_index("ch")
    block, ch, _, nz = x_ref.shape
    parts = nz // LANES
    groups = my // nsub
    half = my * ch
    mx = every.shape[1]
    far = pens // near
    nx = wide.shape[1] // ch
    nblocks = recv.shape[0]
    bunch = recv.shape[2]
    together = bunch // block
    slabs = nblocks * bunch
    chunks = grecv_sem.shape[1]
    span = mx // chunks

    def field_copy(at):
        window = pl.ds(at * bunch, bunch)
        return pltpu.make_async_remote_copy(
            src_ref=feat_ref.at[window],
            dst_ref=field_ref.at[window],
            send_sem=fsend_sem.at[at],
            recv_sem=frecv_sem.at[at],
            device_id={"ch": 1 - core},
            device_id_type=MESH,
        )

    def modes_copy(at, shift, source):
        target = lax.rem(me + shift, pens)
        return pltpu.make_async_remote_copy(
            src_ref=send.at[at, target],
            dst_ref=recv.at[at, source],
            send_sem=send_sem.at[at, shift - 1],
            recv_sem=recv_sem.at[source, at],
            device_id={"pen": target},
            device_id_type=MESH,
        )

    def column_copy(chunk, shift, source):
        target = lax.rem(me + shift * near, pens)
        window = pl.ds(chunk * span, span)
        return pltpu.make_async_remote_copy(
            src_ref=every.at[me, window],
            dst_ref=every.at[source, window],
            send_sem=gsend_sem.at[chunk, shift - 1],
            recv_sem=grecv_sem.at[source, chunk],
            device_id={"pen": target},
            device_id_type=MESH,
        )

    def row_copy(chunk, shift, source, landing):
        base = me - lax.rem(me, near)
        target = base + lax.rem(me + shift, near)
        window = pl.ds(chunk * span, span)
        return pltpu.make_async_remote_copy(
            src_ref=every.at[source, window],
            dst_ref=every.at[landing, window],
            send_sem=psend_sem.at[source, chunk, shift - 1],
            recv_sem=grecv_sem.at[landing, chunk],
            device_id={"pen": target},
            device_id_type=MESH,
        )

    def weight_copy():
        return pltpu.make_async_copy(weight_ref.at[0], weight, wsem)

    def pair_copy():
        return pltpu.make_async_remote_copy(
            src_ref=fx.at[0],
            dst_ref=fx.at[1],
            send_sem=xsem.at[0],
            recv_sem=xsem.at[1],
            device_id={"ch": 1 - core},
            device_id_type=MESH,
        )

    @pl.when(step == 0)
    def _():
        barrier = pltpu.get_barrier_semaphore()
        for shift in range(1, pens):
            pl.semaphore_signal(
                barrier, inc=1, device_id={"pen": lax.rem(me + shift, pens)}, device_id_type=MESH
            )
        pl.semaphore_signal(barrier, inc=1, device_id={"ch": 1 - core}, device_id_type=MESH)
        pl.semaphore_wait(barrier, pens)
        for at in range(nblocks):
            field_copy(at).start()
        weight_copy().start()

    for b in range(block):
        for c in range(ch):
            both = dot(ty_ref[...], x_ref[b, c])
            rows = both[: 2 * my] + both[2 * my :]
            for part in range(parts):
                y_ref[b, part, pl.ds(c, 2 * my, stride=ch), :] = rows[
                    :, part * LANES : (part + 1) * LANES
                ]
    highs, lows = [], []
    for b in range(block):
        pieces = []
        for cs in range(2):
            loaded = [
                y_ref[b, part, cs * half : (cs + 1) * half, :].reshape(groups, nsub, ch, LANES)
                for part in range(parts)
            ]
            for sub in range(nsub):
                for part in range(parts):
                    pieces.append(loaded[part][:, sub].reshape(groups * ch, LANES))
        high, low = split(jnp.concatenate(pieces, axis=1))
        highs.append(high)
        lows.append(low)
    high = jnp.concatenate(highs, axis=0)
    low = jnp.concatenate(lows, axis=0)
    result = dot(high, bh_ref[...]) + dot(low, bh_ref[...]) + dot(high, bl_ref[...])
    result = encode(result, *modes_code).reshape(block, groups, ch, 2 * LANES)
    group, turn = step // together, step % together
    for b in range(block):
        send[group, :, turn * block + b] = result[b]

    @pl.when(turn == together - 1)
    def _():
        recv[group, me] = send[group, me]
        for away in range(1, pens):
            shift = pens // 2 + (away // 2 if away % 2 else -(away // 2))
            modes_copy(group, shift, me).start()

    @pl.when(step == steps - 1)
    def _():
        @pl.loop(0, nblocks)
        def _(at):
            for shift in range(1, pens):
                modes_copy(at, shift, lax.rem(me + pens - shift, pens)).wait_recv()
            rows = decode(recv[at].reshape(pens, bunch * ch, 2 * LANES), *modes_code)
            for source in range(pens):
                start = pl.multiple_of((source * nblocks + at) * (bunch * ch), 8)
                wide[0, pl.ds(start, bunch * ch), :] = rows[source, :, :LANES]
                wide[1, pl.ds(start, bunch * ch), :] = rows[source, :, LANES:]

        for c in range(ch):
            rows = jnp.concatenate(
                [wide[part, pl.ds(c, nx, stride=ch), :] for part in range(2)], axis=1
            )
            high, low = split(rows)
            both = dot(tx_ref[...], jnp.concatenate([high, low], axis=0))
            waves = both[: 2 * mx] + both[2 * mx :]
            fx[0, 0, pl.ds(c, mx, stride=ch), :] = waves[:mx, :LANES] + waves[mx:, LANES:]
            fx[0, 1, pl.ds(c, mx, stride=ch), :] = waves[:mx, LANES:] - waves[mx:, :LANES]
        pair_copy().start()
        weight_copy().wait()

        def mix(slot, j, real, imag):
            first = (core if slot == 0 else 1 - core) * ch
            for c in range(ch):
                x_re = fx[slot, 0, pl.ds(j * ch + c, 1), :]
                x_im = fx[slot, 1, pl.ds(j * ch + c, 1), :]
                w_re = weight[0, j, first + c].astype(F32)
                w_im = weight[1, j, first + c].astype(F32)
                real = real + (x_re * w_re - x_im * w_im)
                imag = imag + (x_im * w_re + x_re * w_im)
            return real, imag

        @pl.loop(0, mx)
        def _(j):
            zero = jnp.zeros(partial.shape[2:], F32)
            partial[0, j], partial[1, j] = mix(0, j, zero, zero)

        pair_copy().wait()

        @pl.loop(0, chunks)
        def _(chunk):
            @pl.loop(0, span)
            def _(local_j):
                j = chunk * span + local_j
                real, imag = mix(1, j, partial[0, j], partial[1, j])
                coded = encode(jnp.concatenate([real, imag], axis=1), *mixed_code)
                every[me, j] = coded

            for shift in range(1, far):
                column_copy(chunk, shift, me).start()
            for shift in range(1, near):
                row_copy(chunk, shift, me, me).start()

        @pl.loop(0, nblocks)
        def _(at):
            for shift in range(1, pens):
                modes_copy(at, shift, me).wait_send()

        x_back = ix_ref[pl.ds(pl.multiple_of(me * slabs, 8), slabs), :]

        def finish(source):
            rows = decode(every[source].reshape(mx * ch, 2 * LANES), *mixed_code)
            plain[0] = rows[:, :LANES]
            plain[1] = rows[:, LANES:]

            for o in range(ch):
                real = plain[0, pl.ds(o, mx, stride=ch), :]
                imag = plain[1, pl.ds(o, mx, stride=ch), :]
                rows = jnp.concatenate(
                    [
                        jnp.concatenate([real, imag], axis=1),
                        jnp.concatenate([imag, -real], axis=1),
                    ],
                    axis=0,
                )
                high, low = split(rows)
                waves = dot(x_back, jnp.concatenate([high, high, low], axis=0))
                window = pl.ds(o * groups + source, slabs, stride=groups * ch)
                out_ref[0, window, :] = waves[:, :LANES]
                out_ref[1, window, :] = waves[:, LANES:]

        finish(me)

        @pl.loop(0, chunks)
        def _(chunk):
            for shift in range(1, far):
                source = lax.rem(me + pens - shift * near, pens)
                column_copy(chunk, shift, source).wait_recv()
                for side in range(1, near):
                    row_copy(chunk, side, source, source).start()

        @pl.loop(1, far)
        def _(shift):
            finish(lax.rem(me + pens - shift * near, pens))

        base = me - lax.rem(me, near)
        for side in range(1, near):
            @pl.loop(0, far)
            def _(shift):
                column = base + lax.rem(me + near - side, near)
                source = lax.rem(column + pens - shift * near, pens)

                @pl.loop(0, chunks)
                def _(chunk):
                    row_copy(chunk, side, source, source).wait_recv()

                finish(source)

        @pl.loop(0, chunks)
        def _(chunk):
            for shift in range(1, far):
                column_copy(chunk, shift, me).wait_send()
            for shift in range(far):
                source = lax.rem(me + pens - shift * near, pens)
                for side in range(1, near):
                    row_copy(chunk, side, source, source).wait_send()

        @pl.loop(0, nblocks)
        def _(at):
            field_copy(at).wait()


def forward_tables(ny, nz, my, mz):
    nsub = LANES // mz
    cos_y, sin_y = tables(ny, my)
    cos_z, sin_z = tables(nz, mz)
    y_table = np.concatenate(split_np(np.concatenate([cos_y, sin_y]) * ny**-0.5), axis=0)
    pair = np.stack([np.stack([cos_z, -sin_z]), np.stack([-sin_z, -cos_z])]) * nz**-0.5
    z_table = np.einsum("crkz,st->cszrtk", pair, np.eye(nsub)).reshape(2 * nsub * nz, 2 * LANES)
    return (y_table, *split_np(z_table))


def inverse_x_table(nx, mx):
    cos_x, sin_x = tables(nx, mx)
    high, low = split_np(np.concatenate([cos_x, -sin_x]).T * mx**-0.5)
    return np.concatenate([high, low, high], axis=1)


def spectrum(features, weights, my, mz, pens, near):
    slabs, ch, ny, nz = features.shape
    _, _, mx, all_ch, _, _ = weights.shape
    nx = slabs * pens
    nsub = LANES // mz
    groups = my // nsub
    y_table, z_high, z_low = forward_tables(ny, nz, my, mz)
    cos_x, sin_x = tables(nx, mx)
    x_high, x_low = split_np(np.concatenate([cos_x, sin_x]) * nx**-0.5)
    x_table = np.concatenate(
        [
            np.concatenate([x_high, x_high], axis=1),
            np.concatenate([x_low, np.zeros_like(x_low)], axis=1),
        ],
        axis=0,
    )
    block = 2 if slabs % 2 == 0 else 1
    steps = slabs // block
    together = TOGETHER if steps % TOGETHER == 0 else 1
    bunch = together * block
    nblocks = steps // together
    chunks = CHUNKS if mx % CHUNKS == 0 else 1
    anywhere = pl.BlockSpec(memory_space=pl.ANY)
    return pl.pallas_call(
        functools.partial(
            spectrum_kernel, my=my, nsub=nsub, pens=pens, near=near,
            modes_code=code_of(9, FIELD_MAX * math.sqrt(ny * nz)),
            mixed_code=code_of(
                7, all_ch * WEIGHT_MAX * math.sqrt(2.0) * FIELD_MAX * math.sqrt(nx * ny * nz)
            ),
        ),
        grid=(steps,),
        in_specs=[
            pl.BlockSpec((block, ch, ny, nz), lambda i: (i, 0, 0, 0)),
            anywhere,
            anywhere,
            whole_vmem(),
            whole_vmem(),
            whole_vmem(),
            whole_vmem(),
            whole_vmem(),
        ],
        out_specs=[whole_vmem(), anywhere],
        out_shape=[
            jax.ShapeDtypeStruct((2, slabs * ch * groups, LANES), F32),
            jax.ShapeDtypeStruct(features.shape, features.dtype),
        ],
        scratch_shapes=[
            pltpu.VMEM((block, nz // LANES, 2 * my * ch, LANES), F32),
            pltpu.VMEM((nblocks, pens, bunch, ch, 2 * LANES), WIRE),
            pltpu.VMEM((nblocks, pens, bunch, ch, 2 * LANES), WIRE),
            pltpu.VMEM((2, nx * ch, LANES), F32),
            pltpu.VMEM((2, 2, mx * ch, LANES), F32),
            pltpu.VMEM((2, mx, all_ch, ch, LANES), BF16),
            pltpu.VMEM((2, mx, ch, LANES), F32),
            pltpu.VMEM((pens, mx, ch, 2 * LANES), WIRE),
            pltpu.VMEM((2, mx * ch, LANES), F32),
            pltpu.SemaphoreType.DMA((nblocks, pens - 1)),
            pltpu.SemaphoreType.DMA((pens, nblocks)),
            pltpu.SemaphoreType.DMA((chunks, max(pens // near - 1, 1))),
            pltpu.SemaphoreType.DMA((pens, chunks)),
            pltpu.SemaphoreType.DMA((pens, chunks, max(near - 1, 1))),
            pltpu.SemaphoreType.DMA((nblocks,)),
            pltpu.SemaphoreType.DMA((nblocks,)),
            pltpu.SemaphoreType.DMA((2,)),
            pltpu.SemaphoreType.DMA,
        ],
        compiler_params=pltpu.CompilerParams(
            vmem_limit_bytes=60 * 2**20, collective_id=0, has_side_effects=True
        ),
        cost_estimate=pl.CostEstimate(
            flops=32 * slabs * ch * my * ny * nz, bytes_accessed=8 * features.size, transcendentals=0
        ),
        name="spectrum",
    )(
        features,
        features,
        weights,
        jnp.asarray(y_table),
        jnp.asarray(z_high),
        jnp.asarray(z_low),
        jnp.asarray(x_table),
        jnp.asarray(inverse_x_table(nx, mx)),
    )


def inverse_kernel(
    start_ref, h_ref, x_ref, peer_ref, mix_ref, rows_ref, cols_ref, mask_ref, bias_ref, ty_ref, tz_ref, out_ref,
    table, shift, even, odd,
    *, nsub, groups, ysub
):
    step = pl.program_id(0)
    _, ch, ny, nz = x_ref.shape
    count = LANES // MZ
    rows = ch * groups
    scale = math.sqrt(2.0 / math.pi)

    def prepare():
        core = lax.axis_index("ch")
        for at, part in enumerate(split(mix_ref[0])):
            wide = lax.dot_general(
                rows_ref[...], part, (((1,), (1,)), ((), ())), preferred_element_type=F32
            )
            wide = dot(wide.astype(BF16), cols_ref[core]) * mask_ref[...]
            half = cols_ref.shape[2]
            table[:, at * half : (at + 1) * half] = wide.astype(BF16)
        lane = lax.broadcasted_iota(jnp.int32, shift.shape[1:], 1)
        row = lax.broadcasted_iota(jnp.int32, shift.shape[1:], 0)
        for o in range(ch):
            high, low = split(jnp.full(shift.shape[1:], bias_ref[0, o] * MZ**0.5, F32))
            value = jnp.where(row == 0, high.astype(F32), low.astype(F32))
            value = jnp.where((row < 2) & (lane % (2 * MZ) == 0), value, 0.0)
            shift[o] = value.astype(BF16)

    def layout(ref):
        real, imag = ref[0], ref[1]
        block = lax.broadcasted_iota(jnp.int32, (rows, LANES), 1) // MZ

        def rolled(value):
            return [value] + [pltpu.roll(value, MZ * at, 1) for at in range(1, count)]

        reals, imags = rolled(real), rolled(imag)
        minus = [-value for value in reals]

        def laid(first, second, sub):
            result = first[-sub % count]
            for at in range(1, count):
                source = (second if at % 2 else first)[(at - sub) % count]
                result = jnp.where(block == at, source, result)
            return result

        tops = [laid(reals, imags, sub) for sub in range(nsub)]
        return tops + [laid(imags, minus, sub) for sub in range(nsub)]

    def along_y(pieces, o):
        window = slice(o * groups, (o + 1) * groups)
        high, low = split(jnp.concatenate([value[window] for value in pieces], axis=0))
        return jnp.concatenate([high, high, low, shift[o]], axis=0)

    def spectral_pair(pieces, pair):
        sides = [along_y(pieces, pair), along_y(pieces, pair + 1)]
        return dot(ty_ref[...], jnp.concatenate(sides, axis=1))

    def spectral_one(waves, at, o, target):
        high, low = split(waves[:, at * LANES : (at + 1) * LANES])
        target[o] = dot(jnp.concatenate([high, low], axis=1), tz_ref[...])

    def bypass(at):
        window = slice(at, at + ysub)
        cells = [ref[0, c, window, :] for ref in (x_ref, peer_ref) for c in range(ch)]
        return dot(table[...], jnp.concatenate(cells + cells, axis=0))

    def activate(at, product, source):
        window = slice(at, at + ysub)
        half = product.reshape(ch, ysub, nz) + source[:, window, :]
        own = x_ref[0, :, window, :].astype(F32)
        cubic = half * (2.0 * scale + (8.0 * 0.044715 * scale) * (half * half))
        out_ref[0, :, window, :] = (half + half * jnp.tanh(cubic)) + own

    @pl.when(step == 0)
    def _():
        prepare()
        pieces = layout(start_ref)
        for pair in range(0, ch, 2):
            waves = spectral_pair(pieces, pair)
            for at in range(2):
                spectral_one(waves, at, pair + at, even)

    def advance(source, target):
        pieces = layout(h_ref)
        turns = ny // ysub
        per = max(ch // turns, 1)
        spaced = max(turns // ch, 1)
        queue = {}
        queue[0] = spectral_pair(pieces, 0)
        product = bypass(0)
        done = 0
        for turn in range(turns):
            if turn % spaced == 0:
                for _ in range(per):
                    if done < ch:
                        pair = done - done % 2
                        if done % 2 == 0 and pair + 2 < ch:
                            queue[pair + 2] = spectral_pair(pieces, pair + 2)
                        spectral_one(queue[pair], done % 2, done, target)
                        done += 1
            following = bypass((turn + 1) * ysub) if turn + 1 < turns else None
            activate(turn * ysub, product, source)
            product = following

    @pl.when(step % 2 == 0)
    def _():
        advance(even, odd)

    @pl.when(step % 2 == 1)
    def _():
        advance(odd, even)


def whole_vmem():
    return pl.BlockSpec(memory_space=pltpu.VMEM)


def forward_modes(features, my, mz):
    slabs, ch, ny, nz = features.shape
    nsub = LANES // mz
    groups = my // nsub
    cos_y, sin_y = tables(ny, my)
    cos_z, sin_z = tables(nz, mz)
    y_table = np.concatenate(split_np(np.concatenate([cos_y, sin_y]) * ny**-0.5), axis=0)
    pair = np.stack([np.stack([cos_z, -sin_z]), np.stack([-sin_z, -cos_z])]) * nz**-0.5
    z_table = np.einsum("crkz,st->cszrtk", pair, np.eye(nsub)).reshape(2 * nsub * nz, 2 * LANES)
    z_high, z_low = split_np(z_table)
    block = 2 if slabs % 2 == 0 else 1
    return pl.pallas_call(
        functools.partial(forward_kernel, my=my, nsub=nsub),
        grid=(slabs // block,),
        in_specs=[
            pl.BlockSpec((block, ch, ny, nz), lambda i: (i, 0, 0, 0)),
            whole_vmem(),
            whole_vmem(),
            whole_vmem(),
        ],
        out_specs=pl.BlockSpec((groups, block, ch, 2 * LANES), lambda i: (0, i, 0, 0)),
        out_shape=jax.ShapeDtypeStruct((groups, slabs, ch, 2 * LANES), F32),
        scratch_shapes=[pltpu.VMEM((block, nz // LANES, 2 * my * ch, LANES), F32)],
        compiler_params=pltpu.CompilerParams(vmem_limit_bytes=48 * 2**20),
        cost_estimate=pl.CostEstimate(
            flops=32 * slabs * ch * my * ny * nz, bytes_accessed=8 * features.size, transcendentals=0
        ),
        name="forward_modes",
    )(features, jnp.asarray(y_table), jnp.asarray(z_high), jnp.asarray(z_low))


def inverse_field(waves, features, peer, mixing, bias, my, mz):
    slabs, ch, ny, nz = features.shape
    all_ch = mixing.shape[1]
    nsub = LANES // mz
    groups = my // nsub
    ysub = YSUB
    rows = ch * groups
    cos_y, sin_y = tables(ny, my)
    cos_z, sin_z = tables(nz, mz)
    y_pair = np.stack([cos_y, -sin_y]).reshape(2, groups, nsub, ny) * my**-0.5
    y_high, y_low = split_np(y_pair.transpose(3, 0, 2, 1).reshape(ny, 2 * my))
    ones = np.zeros((ny, 16), y_high.dtype)
    ones[:, :2] = 1
    y_table = np.concatenate([y_high, y_low, y_high, ones], axis=1)
    z_high, z_low = split_np(np.concatenate([cos_z, -sin_z]) * (0.5 * mz**-0.5))
    copies = LANES // (2 * mz)
    none = np.zeros_like(z_high)
    blank = [none] * (copies - 2)
    z_table = np.concatenate([z_high, z_low, *blank, z_high, none, *blank], axis=0)
    spread_rows = np.repeat(np.eye(ch), ysub, axis=0).astype(ml_dtypes.bfloat16)
    order = np.arange(all_ch)
    spread_cols = np.stack(
        [
            np.repeat((order[:, None] == np.roll(order, -core * ch)[None, :]), ysub, axis=1)
            for core in range(2)
        ]
    ).astype(ml_dtypes.bfloat16)
    mask = (0.5 * np.tile(np.eye(ysub), (ch, all_ch))).astype(np.float32)
    return pl.pallas_call(
        functools.partial(inverse_kernel, nsub=nsub, groups=groups, ysub=ysub),
        grid=(slabs,),
        in_specs=[
            pl.BlockSpec((2, rows, LANES), lambda i: (0, 0, 0)),
            pl.BlockSpec((2, rows, LANES), lambda i: (0, jnp.minimum(i + 1, slabs - 1), 0)),
            pl.BlockSpec((1, ch, ny, nz), lambda i: (i, 0, 0, 0)),
            pl.BlockSpec((1, ch, ny, nz), lambda i: (i, 0, 0, 0)),
            whole_vmem(),
            whole_vmem(),
            whole_vmem(),
            whole_vmem(),
            pl.BlockSpec(memory_space=pltpu.SMEM),
            whole_vmem(),
            whole_vmem(),
        ],
        out_specs=pl.BlockSpec((1, ch, ny, nz), lambda i: (i, 0, 0, 0)),
        out_shape=jax.ShapeDtypeStruct((slabs, ch, ny, nz), F32),
        scratch_shapes=[
            pltpu.VMEM((ch * ysub, 2 * all_ch * ysub), BF16),
            pltpu.VMEM((ch, 16, LANES), BF16),
            pltpu.VMEM((ch, ny, nz), F32),
            pltpu.VMEM((ch, ny, nz), F32),
        ],
        compiler_params=pltpu.CompilerParams(vmem_limit_bytes=48 * 2**20),
        name="inverse_field",
    )(
        waves,
        waves,
        features,
        peer,
        mixing,
        jnp.asarray(spread_rows),
        jnp.asarray(spread_cols),
        jnp.asarray(mask),
        bias,
        jnp.asarray(y_table),
        jnp.asarray(z_table),
    )


YSUB = 8


def spread_spectrum(features, spectral_weights, my, mz, pens):
    slabs, ch, _, _ = features.shape
    _, _, mx, _, _, owned = spectral_weights.shape
    nx = slabs * pens
    groups = my * mz // LANES
    modes = forward_modes(features, my, mz)
    modes = modes.reshape(groups, slabs, ch, 2, LANES).transpose(1, 2, 3, 0, 4)
    modes = modes.reshape(slabs, ch, 2, pens, owned).transpose(3, 0, 1, 2, 4)
    modes = modes.reshape(pens, slabs, ch, 2 * owned)
    modes = lax.all_to_all(modes, "pen", split_axis=0, concat_axis=0, tiled=True)
    modes = modes.reshape(nx, ch, 2 * owned)
    cos_x, sin_x = tables(nx, mx)
    forward_x = jnp.asarray((np.concatenate([cos_x, sin_x]) * nx**-0.5).astype(np.float32))
    waves = jnp.einsum("dx,xcl->dcl", forward_x, modes, precision=HIGHEST)
    real_x = waves[:mx, :, :owned] + waves[mx:, :, owned:]
    imag_x = waves[:mx, :, owned:] - waves[mx:, :, :owned]
    joined = lax.all_gather(
        jnp.concatenate([real_x, imag_x], axis=2), "ch", axis=1, tiled=True
    )
    real_x = joined[:, :, None, :owned]
    imag_x = joined[:, :, None, owned:]
    weight_re = spectral_weights[0, 0].astype(F32)
    weight_im = spectral_weights[0, 1].astype(F32)
    real_g = jnp.sum(real_x * weight_re - imag_x * weight_im, axis=1)
    imag_g = jnp.sum(imag_x * weight_re + real_x * weight_im, axis=1)
    mixed = lax.all_gather(jnp.concatenate([real_g, imag_g], axis=2), "pen", axis=0)
    mixed = mixed.reshape(pens, mx, ch, 2, owned).transpose(1, 2, 3, 0, 4)
    mixed = mixed.reshape(mx, ch, 2, groups, LANES).transpose(3, 0, 1, 2, 4)
    mixed = mixed.reshape(groups, mx, ch, 2, LANES)
    table = inverse_x_table(nx, mx)[:, : 2 * mx].astype(np.float32)
    table = table + inverse_x_table(nx, mx)[:, 2 * mx : 4 * mx].astype(np.float32)
    table = lax.dynamic_slice_in_dim(
        jnp.asarray(table), lax.axis_index("pen") * slabs, slabs, 0
    )
    real, imag = mixed[:, :, :, 0], mixed[:, :, :, 1]
    pair = jnp.stack([jnp.concatenate([real, imag], 1), jnp.concatenate([imag, -real], 1)])
    waves = jnp.einsum("xj,pgjol->pxogl", table, pair, precision=HIGHEST)
    return waves.reshape(2, slabs * ch * groups, LANES)


def local(features, spectral_weights, bypass_weights, bypass_bias, *, pens, kept):
    slabs, ch, _, _ = features.shape
    _, _, mx, all_ch, _, owned = spectral_weights.shape
    mz = MZ
    my = kept // mz
    near = 2 if pens % 2 == 0 else 1
    if owned == LANES and all_ch == 2 * ch:
        waves, peer = spectrum(features, spectral_weights, my, mz, pens, near)
    else:
        peer = lax.ppermute(features, "ch", [(0, 1), (1, 0)])
        waves = spread_spectrum(features, spectral_weights, my, mz, pens)
    return inverse_field(waves, features, peer, bypass_weights, bypass_bias, my, mz)


def solution(mesh):
    pens = mesh.shape["pen"]

    def run(features, spectral_weights, bypass_weights, bypass_bias):
        body = functools.partial(local, pens=pens, kept=spectral_weights.shape[5])
        return jax.shard_map(
            body,
            mesh=mesh,
            in_specs=(
                P(("grp", "pen"), "ch", None, None),
                P(None, None, None, None, "ch", "pen"),
                P(None, None, "ch"),
                P(None, "ch"),
            ),
            out_specs=P(("grp", "pen"), "ch", None, None),
            check_vma=False,
        )(features, spectral_weights, bypass_weights, bypass_bias)

    return run
```

```python
import functools
import math

import jax
import jax.numpy as jnp
import ml_dtypes
import numpy as np
from jax import lax
from jax.experimental import pallas as pl
from jax.experimental.pallas import tpu as pltpu
from jax.sharding import PartitionSpec as P

HIGHEST = lax.Precision.HIGHEST
LANES = 128
MZ = 32
F32 = jnp.float32
BF16 = jnp.bfloat16


def tables(length, kept):
    offsets = np.arange(kept)
    freqs = np.where(offsets < kept // 2, offsets, length - kept + offsets)
    phases = (freqs[:, None] * np.arange(length)[None, :]) % length
    angles = phases.astype(np.float64) * (2.0 * math.pi / length)
    return np.cos(angles), np.sin(angles)


def split_np(table):
    table = table.astype(np.float32)
    high = table.astype(ml_dtypes.bfloat16)
    low = (table - high.astype(np.float32)).astype(ml_dtypes.bfloat16)
    return high, low


def split(value):
    high = value.astype(BF16)
    return high, (value - high.astype(F32)).astype(BF16)


def dot(left, right):
    return jnp.dot(left, right, preferred_element_type=F32)


def forward_kernel(x_ref, ty_ref, bh_ref, bl_ref, out_ref, y_ref, *, my, nsub):
    block, ch, _, nz = x_ref.shape
    parts = nz // LANES
    groups = my // nsub
    half = my * ch
    for b in range(block):
        for c in range(ch):
            both = dot(ty_ref[...], x_ref[b, c])
            rows = both[: 2 * my] + both[2 * my :]
            for part in range(parts):
                y_ref[b, part, pl.ds(c, 2 * my, stride=ch), :] = rows[
                    :, part * LANES : (part + 1) * LANES
                ]
    highs, lows = [], []
    for b in range(block):
        pieces = []
        for cs in range(2):
            loaded = [
                y_ref[b, part, cs * half : (cs + 1) * half, :].reshape(groups, nsub, ch, LANES)
                for part in range(parts)
            ]
            for sub in range(nsub):
                for part in range(parts):
                    pieces.append(loaded[part][:, sub].reshape(groups * ch, LANES))
        high, low = split(jnp.concatenate(pieces, axis=1))
        highs.append(high)
        lows.append(low)
    high = jnp.concatenate(highs, axis=0)
    low = jnp.concatenate(lows, axis=0)
    result = dot(high, bh_ref[...]) + dot(low, bh_ref[...]) + dot(high, bl_ref[...])
    result = result.reshape(block, groups, ch, 2 * LANES)
    for b in range(block):
        out_ref[:, b] = result[b]


MESH = pl.DeviceIdType.MESH
CHUNKS = 2
TOGETHER = 1


def odd_power(value, power):
    result, square = value, value * value
    while power > 1:
        result, power = result * square, power - 2
    return result


def encode(value, power, scale):
    return odd_power(value * scale, power).astype(WIRE)


def decode(code, power, scale):
    code = code.astype(F32)
    root = jnp.exp2(jnp.log2(jnp.abs(code)) * (1.0 / power)) * (1.0 / scale)
    return jnp.where(code < 0.0, -root, root)


WIRE = BF16
FIELD_MAX = 6.0
WEIGHT_MAX = 0.75


def code_of(power, bound):
    reach = 2.0 ** (126.0 / power)
    return power, 2.0 ** math.floor(math.log2(reach / bound))


def spectrum_kernel(
    x_ref, feat_ref, weight_ref, ty_ref, bh_ref, bl_ref, tx_ref, ix_ref, out_ref, field_ref,
    tables_ref, y_ref, send, recv, wide, fx, weight, partial, every, plain,
    send_sem, recv_sem, gsend_sem, grecv_sem, psend_sem, fsend_sem, frecv_sem, xsem, wsem, tsem,
    *, my, nsub, pens, near, modes_code, mixed_code,
):
    step = pl.program_id(0)
    steps = pl.num_programs(0)
    me = lax.axis_index("pen")
    core = lax.axis_index("ch")
    block, ch, _, nz = x_ref.shape
    parts = nz // LANES
    groups = my // nsub
    mx = every.shape[1]
    far = pens // near
    nx = wide.shape[1] // ch
    nblocks = recv.shape[0]
    bunch = recv.shape[2]
    together = bunch // block
    slabs = nblocks * bunch
    chunks = grecv_sem.shape[1]
    span = mx // chunks

    def field_copy(at):
        window = pl.ds(at * bunch, bunch)
        return pltpu.make_async_remote_copy(
            src_ref=feat_ref.at[window],
            dst_ref=field_ref.at[window],
            send_sem=fsend_sem.at[at],
            recv_sem=frecv_sem.at[at],
            device_id={"ch": 1 - core},
            device_id_type=MESH,
        )

    def modes_copy(at, shift, source):
        target = lax.rem(me + shift, pens)
        return pltpu.make_async_remote_copy(
            src_ref=send.at[at, target],
            dst_ref=recv.at[at, source],
            send_sem=send_sem.at[at, shift - 1],
            recv_sem=recv_sem.at[source, at],
            device_id={"pen": target},
            device_id_type=MESH,
        )

    def column_copy(chunk, shift, source):
        target = lax.rem(me + shift * near, pens)
        window = pl.ds(chunk * span, span)
        return pltpu.make_async_remote_copy(
            src_ref=every.at[me, window],
            dst_ref=every.at[source, window],
            send_sem=gsend_sem.at[chunk, shift - 1],
            recv_sem=grecv_sem.at[source, chunk],
            device_id={"pen": target},
            device_id_type=MESH,
        )

    def row_copy(chunk, shift, source, landing):
        base = me - lax.rem(me, near)
        target = base + lax.rem(me + shift, near)
        window = pl.ds(chunk * span, span)
        return pltpu.make_async_remote_copy(
            src_ref=every.at[source, window],
            dst_ref=every.at[landing, window],
            send_sem=psend_sem.at[source, chunk, shift - 1],
            recv_sem=grecv_sem.at[landing, chunk],
            device_id={"pen": target},
            device_id_type=MESH,
        )

    def weight_copy():
        return pltpu.make_async_copy(weight_ref.at[0], weight, wsem)

    def table_copy(at):
        source = (bh_ref, bl_ref)[at]
        return pltpu.make_async_copy(source, tables_ref.at[at], tsem.at[at])

    def pair_copy():
        return pltpu.make_async_remote_copy(
            src_ref=fx.at[0],
            dst_ref=fx.at[1],
            send_sem=xsem.at[0],
            recv_sem=xsem.at[1],
            device_id={"ch": 1 - core},
            device_id_type=MESH,
        )

    @pl.when(step == 0)
    def _():
        for at in range(2):
            table_copy(at).start()
        barrier = pltpu.get_barrier_semaphore()
        for shift in range(1, pens):
            pl.semaphore_signal(
                barrier, inc=1, device_id={"pen": lax.rem(me + shift, pens)}, device_id_type=MESH
            )
        pl.semaphore_signal(barrier, inc=1, device_id={"ch": 1 - core}, device_id_type=MESH)
        weight_copy().start()

    tall = ty_ref.shape[0] // 2
    top = my // 2
    for b in range(block):
        for c in range(ch):
            both = dot(ty_ref[...], x_ref[b, c])
            rows = both[:tall] + both[tall:]
            for part in range(parts):
                y_ref[b, part, pl.ds(c, tall, stride=ch), :] = rows[
                    :, part * LANES : (part + 1) * LANES
                ]

    def wave(b, part, sine, index):
        freq = index if index < top else my - index
        if sine and freq == 0:
            return jnp.zeros((ch, LANES), F32)
        row = (top + freq if sine else freq) * ch
        value = y_ref[b, part, row : row + ch, :]
        return -value if sine and index >= top else value

    highs, lows = [], []
    for b in range(block):
        pieces = [
            jnp.concatenate(
                [wave(b, part, sine, group * nsub + sub) for group in range(groups)], axis=0
            )
            for sine in range(2)
            for sub in range(nsub)
            for part in range(parts)
        ]
        high, low = split(jnp.concatenate(pieces, axis=1))
        highs.append(high)
        lows.append(low)
    high = jnp.concatenate(highs, axis=0)
    low = jnp.concatenate(lows, axis=0)

    @pl.when(step == 0)
    def _():
        pl.semaphore_wait(pltpu.get_barrier_semaphore(), pens)
        for at in range(nblocks):
            field_copy(at).start()
        for at in range(2):
            table_copy(at).wait()

    result = dot(high, tables_ref[0]) + dot(low, tables_ref[0]) + dot(high, tables_ref[1])
    result = encode(result, *modes_code).reshape(block, groups, ch, 2 * LANES)
    group, turn = step // together, step % together
    for b in range(block):
        send[group, :, turn * block + b] = result[b]

    @pl.when(turn == together - 1)
    def _():
        recv[group, me] = send[group, me]
        for away in range(1, pens):
            shift = pens // 2 + (away // 2 if away % 2 else -(away // 2))
            modes_copy(group, shift, me).start()

    @pl.when(step == steps - 1)
    def _():
        @pl.loop(0, nblocks)
        def _(at):
            for shift in range(1, pens):
                modes_copy(at, shift, lax.rem(me + pens - shift, pens)).wait_recv()
            rows = decode(recv[at].reshape(pens, bunch * ch, 2 * LANES), *modes_code)
            for source in range(pens):
                start = pl.multiple_of((source * nblocks + at) * (bunch * ch), 8)
                wide[0, pl.ds(start, bunch * ch), :] = rows[source, :, :LANES]
                wide[1, pl.ds(start, bunch * ch), :] = rows[source, :, LANES:]

        for c in range(ch):
            rows = jnp.concatenate(
                [wide[part, pl.ds(c, nx, stride=ch), :] for part in range(2)], axis=1
            )
            high, low = split(rows)
            both = dot(tx_ref[...], jnp.concatenate([high, low], axis=0))
            waves = both[: 2 * mx] + both[2 * mx :]
            fx[0, 0, pl.ds(c, mx, stride=ch), :] = waves[:mx, :LANES] + waves[mx:, LANES:]
            fx[0, 1, pl.ds(c, mx, stride=ch), :] = waves[:mx, LANES:] - waves[mx:, :LANES]
        pair_copy().start()
        weight_copy().wait()

        def mix(slot, j, real, imag):
            first = (core if slot == 0 else 1 - core) * ch
            for c in range(ch):
                x_re = fx[slot, 0, pl.ds(j * ch + c, 1), :]
                x_im = fx[slot, 1, pl.ds(j * ch + c, 1), :]
                w_re = weight[0, j, first + c].astype(F32)
                w_im = weight[1, j, first + c].astype(F32)
                real = real + (x_re * w_re - x_im * w_im)
                imag = imag + (x_im * w_re + x_re * w_im)
            return real, imag

        @pl.loop(0, mx)
        def _(j):
            zero = jnp.zeros(partial.shape[2:], F32)
            partial[0, j], partial[1, j] = mix(0, j, zero, zero)

        pair_copy().wait()

        @pl.loop(0, chunks)
        def _(chunk):
            @pl.loop(0, span)
            def _(local_j):
                j = chunk * span + local_j
                real, imag = mix(1, j, partial[0, j], partial[1, j])
                coded = encode(jnp.concatenate([real, imag], axis=1), *mixed_code)
                every[me, j] = coded

            for shift in range(1, far):
                column_copy(chunk, shift, me).start()
            for shift in range(1, near):
                row_copy(chunk, shift, me, me).start()

        @pl.loop(0, nblocks)
        def _(at):
            for shift in range(1, pens):
                modes_copy(at, shift, me).wait_send()

        x_back = ix_ref[pl.ds(pl.multiple_of(me * slabs, 8), slabs), :]

        def finish(source):
            rows = decode(every[source].reshape(mx * ch, 2 * LANES), *mixed_code)
            plain[0] = rows[:, :LANES]
            plain[1] = rows[:, LANES:]

            for o in range(ch):
                real = plain[0, pl.ds(o, mx, stride=ch), :]
                imag = plain[1, pl.ds(o, mx, stride=ch), :]
                rows = jnp.concatenate(
                    [
                        jnp.concatenate([real, imag], axis=1),
                        jnp.concatenate([imag, -real], axis=1),
                    ],
                    axis=0,
                )
                high, low = split(rows)
                waves = dot(x_back, jnp.concatenate([high, high, low], axis=0))
                window = pl.ds(o * groups + source, slabs, stride=groups * ch)
                out_ref[0, window, :] = waves[:, :LANES]
                out_ref[1, window, :] = waves[:, LANES:]

        finish(me)

        @pl.loop(0, chunks)
        def _(chunk):
            for shift in range(1, far):
                source = lax.rem(me + pens - shift * near, pens)
                column_copy(chunk, shift, source).wait_recv()
                for side in range(1, near):
                    row_copy(chunk, side, source, source).start()

        @pl.loop(1, far)
        def _(shift):
            finish(lax.rem(me + pens - shift * near, pens))

        base = me - lax.rem(me, near)
        for side in range(1, near):
            @pl.loop(0, far)
            def _(shift):
                column = base + lax.rem(me + near - side, near)
                source = lax.rem(column + pens - shift * near, pens)

                @pl.loop(0, chunks)
                def _(chunk):
                    row_copy(chunk, side, source, source).wait_recv()

                finish(source)

        @pl.loop(0, chunks)
        def _(chunk):
            for shift in range(1, far):
                column_copy(chunk, shift, me).wait_send()
            for shift in range(far):
                source = lax.rem(me + pens - shift * near, pens)
                for side in range(1, near):
                    row_copy(chunk, side, source, source).wait_send()

        @pl.loop(0, nblocks)
        def _(at):
            field_copy(at).wait()


def forward_tables(ny, nz, my, mz):
    nsub = LANES // mz
    cos_y, sin_y = tables(ny, my)
    cos_z, sin_z = tables(nz, mz)
    y_table = np.concatenate(split_np(np.concatenate([cos_y, sin_y]) * ny**-0.5), axis=0)
    pair = np.stack([np.stack([cos_z, -sin_z]), np.stack([-sin_z, -cos_z])]) * nz**-0.5
    z_table = np.einsum("crkz,st->cszrtk", pair, np.eye(nsub)).reshape(2 * nsub * nz, 2 * LANES)
    return (y_table, *split_np(z_table))


def inverse_x_table(nx, mx):
    cos_x, sin_x = tables(nx, mx)
    high, low = split_np(np.concatenate([cos_x, -sin_x]).T * mx**-0.5)
    return np.concatenate([high, low, high], axis=1)


def spectrum(features, weights, my, mz, pens, near):
    slabs, ch, ny, nz = features.shape
    _, _, mx, all_ch, _, _ = weights.shape
    nx = slabs * pens
    nsub = LANES // mz
    groups = my // nsub
    _, z_high, z_low = forward_tables(ny, nz, my, mz)
    top = my // 2
    angles = (np.arange(top + 1)[:, None] * np.arange(ny)[None, :]) % ny * (2.0 * math.pi / ny)
    tall = -(-(my + 1) // 8) * 8
    y_rows = np.zeros((tall, ny))
    y_rows[: my + 1] = np.concatenate([np.cos(angles), np.sin(angles[1:])]) * ny**-0.5
    y_table = np.concatenate(split_np(y_rows), axis=0)
    cos_x, sin_x = tables(nx, mx)
    x_high, x_low = split_np(np.concatenate([cos_x, sin_x]) * nx**-0.5)
    x_table = np.concatenate(
        [
            np.concatenate([x_high, x_high], axis=1),
            np.concatenate([x_low, np.zeros_like(x_low)], axis=1),
        ],
        axis=0,
    )
    block = 2 if slabs % 2 == 0 else 1
    steps = slabs // block
    together = TOGETHER if steps % TOGETHER == 0 else 1
    bunch = together * block
    nblocks = steps // together
    chunks = CHUNKS if mx % CHUNKS == 0 else 1
    anywhere = pl.BlockSpec(memory_space=pltpu.HBM)
    return pl.pallas_call(
        functools.partial(
            spectrum_kernel, my=my, nsub=nsub, pens=pens, near=near,
            modes_code=code_of(9, FIELD_MAX * math.sqrt(ny * nz)),
            mixed_code=code_of(
                7, all_ch * WEIGHT_MAX * math.sqrt(2.0) * FIELD_MAX * math.sqrt(nx * ny * nz)
            ),
        ),
        grid=(steps,),
        in_specs=[
            pl.BlockSpec((block, ch, ny, nz), lambda i: (i, 0, 0, 0)),
            anywhere,
            anywhere,
            whole_vmem(),
            anywhere,
            anywhere,
            whole_vmem(),
            whole_vmem(),
        ],
        out_specs=[whole_vmem(), anywhere],
        out_shape=[
            jax.ShapeDtypeStruct((2, slabs * ch * groups, LANES), F32),
            jax.ShapeDtypeStruct(features.shape, features.dtype),
        ],
        scratch_shapes=[
            pltpu.VMEM((2, *z_high.shape), BF16),
            pltpu.VMEM((block, nz // LANES, tall * ch, LANES), F32),
            pltpu.VMEM((nblocks, pens, bunch, ch, 2 * LANES), WIRE),
            pltpu.VMEM((nblocks, pens, bunch, ch, 2 * LANES), WIRE),
            pltpu.VMEM((2, nx * ch, LANES), F32),
            pltpu.VMEM((2, 2, mx * ch, LANES), F32),
            pltpu.VMEM((2, mx, all_ch, ch, LANES), BF16),
            pltpu.VMEM((2, mx, ch, LANES), F32),
            pltpu.VMEM((pens, mx, ch, 2 * LANES), WIRE),
            pltpu.VMEM((2, mx * ch, LANES), F32),
            pltpu.SemaphoreType.DMA((nblocks, pens - 1)),
            pltpu.SemaphoreType.DMA((pens, nblocks)),
            pltpu.SemaphoreType.DMA((chunks, max(pens // near - 1, 1))),
            pltpu.SemaphoreType.DMA((pens, chunks)),
            pltpu.SemaphoreType.DMA((pens, chunks, max(near - 1, 1))),
            pltpu.SemaphoreType.DMA((nblocks,)),
            pltpu.SemaphoreType.DMA((nblocks,)),
            pltpu.SemaphoreType.DMA((2,)),
            pltpu.SemaphoreType.DMA,
            pltpu.SemaphoreType.DMA((2,)),
        ],
        compiler_params=pltpu.CompilerParams(
            vmem_limit_bytes=64900000, collective_id=0, has_side_effects=True
        ),
        cost_estimate=pl.CostEstimate(
            flops=32 * slabs * ch * my * ny * nz, bytes_accessed=8 * features.size, transcendentals=0
        ),
        name="spectrum",
    )(
        features,
        features,
        weights,
        jnp.asarray(y_table),
        jnp.asarray(z_high),
        jnp.asarray(z_low),
        jnp.asarray(x_table),
        jnp.asarray(inverse_x_table(nx, mx)),
    )


def inverse_kernel(
    start_ref, h_ref, x_ref, peer_ref, mix_ref, rows_ref, cols_ref, mask_ref, bias_ref, ty_ref, tz_ref, out_ref,
    table, shift, even, odd,
    *, nsub, groups, ysub
):
    step = pl.program_id(0)
    _, ch, ny, nz = x_ref.shape
    count = LANES // MZ
    rows = ch * groups
    scale = math.sqrt(2.0 / math.pi)

    def prepare():
        core = lax.axis_index("ch")
        for at, part in enumerate(split(mix_ref[0])):
            wide = lax.dot_general(
                rows_ref[...], part, (((1,), (1,)), ((), ())), preferred_element_type=F32
            )
            wide = dot(wide.astype(BF16), cols_ref[core]) * mask_ref[...]
            half = cols_ref.shape[2]
            table[:, at * half : (at + 1) * half] = wide.astype(BF16)
        lane = lax.broadcasted_iota(jnp.int32, shift.shape[1:], 1)
        row = lax.broadcasted_iota(jnp.int32, shift.shape[1:], 0)
        for o in range(ch):
            high, low = split(jnp.full(shift.shape[1:], bias_ref[0, o] * MZ**0.5, F32))
            value = jnp.where(row == 0, high.astype(F32), low.astype(F32))
            value = jnp.where((row < 2) & (lane % (2 * MZ) == 0), value, 0.0)
            shift[o] = value.astype(BF16)

    def layout(ref):
        real, imag = ref[0], ref[1]
        block = lax.broadcasted_iota(jnp.int32, (rows, LANES), 1) // MZ

        def rolled(value):
            return [value] + [pltpu.roll(value, MZ * at, 1) for at in range(1, count)]

        reals, imags = rolled(real), rolled(imag)
        minus = [-value for value in reals]

        def laid(first, second, sub):
            result = first[-sub % count]
            for at in range(1, count):
                source = (second if at % 2 else first)[(at - sub) % count]
                result = jnp.where(block == at, source, result)
            return result

        tops = [laid(reals, imags, sub) for sub in range(nsub)]
        return tops + [laid(imags, minus, sub) for sub in range(nsub)]

    def along_y(pieces, o):
        window = slice(o * groups, (o + 1) * groups)
        high, low = split(jnp.concatenate([value[window] for value in pieces], axis=0))
        return jnp.concatenate([high, high, low, shift[o]], axis=0)

    def spectral_pair(pieces, pair):
        sides = [along_y(pieces, pair), along_y(pieces, pair + 1)]
        return dot(ty_ref[...], jnp.concatenate(sides, axis=1))

    def spectral_one(waves, at, o, target):
        high, low = split(waves[:, at * LANES : (at + 1) * LANES])
        target[o] = dot(jnp.concatenate([high, low], axis=1), tz_ref[...])

    def bypass(at):
        window = slice(at, at + ysub)
        cells = [ref[0, c, window, :] for ref in (x_ref, peer_ref) for c in range(ch)]
        return dot(table[...], jnp.concatenate(cells + cells, axis=0))

    def activate(at, product, source):
        window = slice(at, at + ysub)
        half = product.reshape(ch, ysub, nz) + source[:, window, :]
        own = x_ref[0, :, window, :].astype(F32)
        cubic = half * (2.0 * scale + (8.0 * 0.044715 * scale) * (half * half))
        out_ref[0, :, window, :] = (half + half * jnp.tanh(cubic)) + own

    @pl.when(step == 0)
    def _():
        prepare()
        pieces = layout(start_ref)
        for pair in range(0, ch, 2):
            waves = spectral_pair(pieces, pair)
            for at in range(2):
                spectral_one(waves, at, pair + at, even)

    def advance(source, target):
        pieces = layout(h_ref)
        turns = ny // ysub
        per = max(ch // turns, 1)
        spaced = max(turns // ch, 1)
        queue = {}
        queue[0] = spectral_pair(pieces, 0)
        product = bypass(0)
        done = 0
        for turn in range(turns):
            if turn % spaced == 0:
                for _ in range(per):
                    if done < ch:
                        pair = done - done % 2
                        if done % 2 == 0 and pair + 2 < ch:
                            queue[pair + 2] = spectral_pair(pieces, pair + 2)
                        spectral_one(queue[pair], done % 2, done, target)
                        done += 1
            following = bypass((turn + 1) * ysub) if turn + 1 < turns else None
            activate(turn * ysub, product, source)
            product = following

    @pl.when(step % 2 == 0)
    def _():
        advance(even, odd)

    @pl.when(step % 2 == 1)
    def _():
        advance(odd, even)


def whole_vmem():
    return pl.BlockSpec(memory_space=pltpu.VMEM)


def forward_modes(features, my, mz):
    slabs, ch, ny, nz = features.shape
    nsub = LANES // mz
    groups = my // nsub
    cos_y, sin_y = tables(ny, my)
    cos_z, sin_z = tables(nz, mz)
    y_table = np.concatenate(split_np(np.concatenate([cos_y, sin_y]) * ny**-0.5), axis=0)
    pair = np.stack([np.stack([cos_z, -sin_z]), np.stack([-sin_z, -cos_z])]) * nz**-0.5
    z_table = np.einsum("crkz,st->cszrtk", pair, np.eye(nsub)).reshape(2 * nsub * nz, 2 * LANES)
    z_high, z_low = split_np(z_table)
    block = 2 if slabs % 2 == 0 else 1
    return pl.pallas_call(
        functools.partial(forward_kernel, my=my, nsub=nsub),
        grid=(slabs // block,),
        in_specs=[
            pl.BlockSpec((block, ch, ny, nz), lambda i: (i, 0, 0, 0)),
            whole_vmem(),
            whole_vmem(),
            whole_vmem(),
        ],
        out_specs=pl.BlockSpec((groups, block, ch, 2 * LANES), lambda i: (0, i, 0, 0)),
        out_shape=jax.ShapeDtypeStruct((groups, slabs, ch, 2 * LANES), F32),
        scratch_shapes=[pltpu.VMEM((block, nz // LANES, 2 * my * ch, LANES), F32)],
        compiler_params=pltpu.CompilerParams(vmem_limit_bytes=48 * 2**20),
        cost_estimate=pl.CostEstimate(
            flops=32 * slabs * ch * my * ny * nz, bytes_accessed=8 * features.size, transcendentals=0
        ),
        name="forward_modes",
    )(features, jnp.asarray(y_table), jnp.asarray(z_high), jnp.asarray(z_low))


def inverse_field(waves, features, peer, mixing, bias, my, mz):
    slabs, ch, ny, nz = features.shape
    all_ch = mixing.shape[1]
    nsub = LANES // mz
    groups = my // nsub
    ysub = YSUB
    rows = ch * groups
    cos_y, sin_y = tables(ny, my)
    cos_z, sin_z = tables(nz, mz)
    y_pair = np.stack([cos_y, -sin_y]).reshape(2, groups, nsub, ny) * my**-0.5
    y_high, y_low = split_np(y_pair.transpose(3, 0, 2, 1).reshape(ny, 2 * my))
    ones = np.zeros((ny, 16), y_high.dtype)
    ones[:, :2] = 1
    y_table = np.concatenate([y_high, y_low, y_high, ones], axis=1)
    z_high, z_low = split_np(np.concatenate([cos_z, -sin_z]) * (0.5 * mz**-0.5))
    copies = LANES // (2 * mz)
    none = np.zeros_like(z_high)
    blank = [none] * (copies - 2)
    z_table = np.concatenate([z_high, z_low, *blank, z_high, none, *blank], axis=0)
    spread_rows = np.repeat(np.eye(ch), ysub, axis=0).astype(ml_dtypes.bfloat16)
    order = np.arange(all_ch)
    spread_cols = np.stack(
        [
            np.repeat((order[:, None] == np.roll(order, -core * ch)[None, :]), ysub, axis=1)
            for core in range(2)
        ]
    ).astype(ml_dtypes.bfloat16)
    mask = (0.5 * np.tile(np.eye(ysub), (ch, all_ch))).astype(np.float32)
    return pl.pallas_call(
        functools.partial(inverse_kernel, nsub=nsub, groups=groups, ysub=ysub),
        grid=(slabs,),
        in_specs=[
            pl.BlockSpec((2, rows, LANES), lambda i: (0, 0, 0)),
            pl.BlockSpec((2, rows, LANES), lambda i: (0, jnp.minimum(i + 1, slabs - 1), 0)),
            pl.BlockSpec((1, ch, ny, nz), lambda i: (i, 0, 0, 0)),
            pl.BlockSpec((1, ch, ny, nz), lambda i: (i, 0, 0, 0)),
            whole_vmem(),
            whole_vmem(),
            whole_vmem(),
            whole_vmem(),
            pl.BlockSpec(memory_space=pltpu.SMEM),
            whole_vmem(),
            whole_vmem(),
        ],
        out_specs=pl.BlockSpec((1, ch, ny, nz), lambda i: (i, 0, 0, 0)),
        out_shape=jax.ShapeDtypeStruct((slabs, ch, ny, nz), F32),
        scratch_shapes=[
            pltpu.VMEM((ch * ysub, 2 * all_ch * ysub), BF16),
            pltpu.VMEM((ch, 16, LANES), BF16),
            pltpu.VMEM((ch, ny, nz), F32),
            pltpu.VMEM((ch, ny, nz), F32),
        ],
        compiler_params=pltpu.CompilerParams(vmem_limit_bytes=60 * 2**20),
        name="inverse_field",
    )(
        waves,
        waves,
        features,
        peer,
        mixing,
        jnp.asarray(spread_rows),
        jnp.asarray(spread_cols),
        jnp.asarray(mask),
        bias,
        jnp.asarray(y_table),
        jnp.asarray(z_table),
    )


YSUB = 8


def spread_spectrum(features, spectral_weights, my, mz, pens):
    slabs, ch, _, _ = features.shape
    _, _, mx, _, _, owned = spectral_weights.shape
    nx = slabs * pens
    groups = my * mz // LANES
    modes = forward_modes(features, my, mz)
    modes = modes.reshape(groups, slabs, ch, 2, LANES).transpose(1, 2, 3, 0, 4)
    modes = modes.reshape(slabs, ch, 2, pens, owned).transpose(3, 0, 1, 2, 4)
    modes = modes.reshape(pens, slabs, ch, 2 * owned)
    modes = lax.all_to_all(modes, "pen", split_axis=0, concat_axis=0, tiled=True)
    modes = modes.reshape(nx, ch, 2 * owned)
    cos_x, sin_x = tables(nx, mx)
    forward_x = jnp.asarray((np.concatenate([cos_x, sin_x]) * nx**-0.5).astype(np.float32))
    waves = jnp.einsum("dx,xcl->dcl", forward_x, modes, precision=HIGHEST)
    real_x = waves[:mx, :, :owned] + waves[mx:, :, owned:]
    imag_x = waves[:mx, :, owned:] - waves[mx:, :, :owned]
    joined = lax.all_gather(
        jnp.concatenate([real_x, imag_x], axis=2), "ch", axis=1, tiled=True
    )
    real_x = joined[:, :, None, :owned]
    imag_x = joined[:, :, None, owned:]
    weight_re = spectral_weights[0, 0].astype(F32)
    weight_im = spectral_weights[0, 1].astype(F32)
    real_g = jnp.sum(real_x * weight_re - imag_x * weight_im, axis=1)
    imag_g = jnp.sum(imag_x * weight_re + real_x * weight_im, axis=1)
    mixed = lax.all_gather(jnp.concatenate([real_g, imag_g], axis=2), "pen", axis=0)
    mixed = mixed.reshape(pens, mx, ch, 2, owned).transpose(1, 2, 3, 0, 4)
    mixed = mixed.reshape(mx, ch, 2, groups, LANES).transpose(3, 0, 1, 2, 4)
    mixed = mixed.reshape(groups, mx, ch, 2, LANES)
    table = inverse_x_table(nx, mx)[:, : 2 * mx].astype(np.float32)
    table = table + inverse_x_table(nx, mx)[:, 2 * mx : 4 * mx].astype(np.float32)
    table = lax.dynamic_slice_in_dim(
        jnp.asarray(table), lax.axis_index("pen") * slabs, slabs, 0
    )
    real, imag = mixed[:, :, :, 0], mixed[:, :, :, 1]
    pair = jnp.stack([jnp.concatenate([real, imag], 1), jnp.concatenate([imag, -real], 1)])
    waves = jnp.einsum("xj,pgjol->pxogl", table, pair, precision=HIGHEST)
    return waves.reshape(2, slabs * ch * groups, LANES)


def local(features, spectral_weights, bypass_weights, bypass_bias, *, pens, kept):
    slabs, ch, _, _ = features.shape
    _, _, mx, all_ch, _, owned = spectral_weights.shape
    mz = MZ
    my = kept // mz
    near = 2 if pens % 2 == 0 else 1
    if owned == LANES and all_ch == 2 * ch:
        waves, peer = spectrum(features, spectral_weights, my, mz, pens, near)
    else:
        peer = lax.ppermute(features, "ch", [(0, 1), (1, 0)])
        waves = spread_spectrum(features, spectral_weights, my, mz, pens)
    return inverse_field(waves, features, peer, bypass_weights, bypass_bias, my, mz)


def solution(mesh):
    pens = mesh.shape["pen"]

    def run(features, spectral_weights, bypass_weights, bypass_bias):
        body = functools.partial(local, pens=pens, kept=spectral_weights.shape[5])
        return jax.shard_map(
            body,
            mesh=mesh,
            in_specs=(
                P(("grp", "pen"), "ch", None, None),
                P(None, None, None, None, "ch", "pen"),
                P(None, None, "ch"),
                P(None, "ch"),
            ),
            out_specs=P(("grp", "pen"), "ch", None, None),
            check_vma=False,
        )(features, spectral_weights, bypass_weights, bypass_bias)

    return run
```
